32 devices in a mesh: groups: 2 (over y), heads: 4 (over z), batch: 4 (over x, core).
Axes of the slice: x: 2, y: 2, z: 4, core: 2. Of those that a mesh axis runs over, the one named last changes fastest.
Arguments:
- queries: bfloat16 [128, 8192], P(('groups', 'batch'), 'heads'), parts along dimension 0, may hold values from -110 to 110
- new_kv: bfloat16 [16, 64, 256], P(('groups', 'heads'), 'batch'), parts along dimension 0, may hold values from -15 to 15
- kv_pool: bfloat16 [16, 192, 128, 256], P(('groups', 'heads'), 'batch'), parts along dimension 0, may hold values from -6 to 6
- page_counts: int32 [8, 16], P(('groups', 'batch')), parts along dimension 0, may hold values from 1 to 6, 48 in all within a row
- last_fill: int32 [8, 16], P(('groups', 'batch')), parts along dimension 0, may hold values from 1 to 128
- page_order: int32 [8, 48], P(('groups', 'batch')), parts along dimension 0, may hold values from 0 to 47, each once within a row
- hidden: bfloat16 [128, 8192], P(('groups', 'batch')), parts along dimension 0, may hold values from -0.59765625 to 0.59765625
- out_weight: bfloat16 [8192, 8192], P('heads'), may hold values from -0.5 to 0.5
- norm_gain: bfloat16 [8192], replicated, may hold values from 0.099609375 to 1.8984375
- sectioned: bfloat16 [8, 4, 8, 128, 256], P(('groups', 'heads'), 'batch'), parts along dimension 0, may hold values from -6 to 6
- routes: int32 [8, 4, 8, 1], P(('groups', 'heads'), 'batch'), parts along dimension 0, may hold values from 0 to 7; in each aligned block of 8 rows (0 to 7, 8 to 15, ..., all dimensions but the last counted through in order) at most 2 rows name the same one
Outputs:
- residual_out: bfloat16 [128, 8192], P(('groups', 'batch')), parts along dimension 0
- normed: bfloat16 [128, 8192], P(('groups', 'batch')), parts along dimension 0
- arrival: bfloat16 [16, 4, 4, 2, 128, 256], P(('groups', 'heads'), 'batch'), parts along dimension 0
The draws below stay inside these ranges and needn't reach their ends.
There are 2 independent parts, one for each index of `groups`. The reference program is written for one: setup_inputs(seed, part) draws one part's arguments, and reference() takes and returns one part's arrays. A program takes and returns all parts, laid end to end along the dimension named above; an argument that names none is the same for every part. Nothing has to cross between parts.
Inputs may be any that keep to these rules, and one draw needn't show every extreme that they name: `routes`: every key-value head is named by at most 2 sectioned pages of one device. `page_counts`: the page counts of one batch owner sum to 48.
All inputs are finite; a program needn't handle non-finite values.
Results may differ from the reference program's by a relative error of at most 0.0066.
Values may be sent and summed in bfloat16 or wider, within the bound.
A program may use at most 128 MiB of HBM per device.

```python
import math
import jax
import jax.numpy as jnp
import numpy as np
from jax import lax

D = 8192
Q_HEADS = 64
KV_HEADS = 8
HEAD_DIM = 128
PAGE = 128
MAX_PAGES = 6
SECTION_DEV = 8
PER_HEAD_CAP = 2
REQ_DEV = 16
KV_WIDTH = 256
CACHE_SLOTS = 8
POOL_DEV = 48
REQUESTS = 64
N_HEADS = 4
N_BATCH = 4


def draw_kv_pool(key, part):
    full_shape = (CACHE_SLOTS, N_BATCH * POOL_DEV, PAGE, 2 * HEAD_DIM)
    base_draw = jnp.clip(jax.random.normal(jax.random.fold_in(key, 101), full_shape, jnp.float32), -6.0, 6.0)
    return base_draw.astype(jnp.bfloat16)


def draw_queries(key, part):
    row_total = N_BATCH * REQ_DEV
    base_draw = jnp.clip(jax.random.normal(jax.random.fold_in(key, 201), (row_total, Q_HEADS, HEAD_DIM), jnp.float32), -6.0, 6.0)
    return base_draw.reshape(row_total, Q_HEADS * HEAD_DIM).astype(jnp.bfloat16)


def draw_out_weight(key, part):
    row_total = Q_HEADS * HEAD_DIM
    common_share = 0.2
    scale_reach = 0.6
    base_draw = jnp.clip(jax.random.normal(jax.random.fold_in(key, 301), (row_total, D), jnp.float32), -4.0, 4.0)
    loadings = jnp.clip(jax.random.normal(jax.random.fold_in(key, 302), (row_total, 1), jnp.float32), -3.0, 3.0)
    common_row = jnp.clip(jax.random.normal(jax.random.fold_in(key, 303), (1, D), jnp.float32), -3.0, 3.0)
    row_scale = jnp.exp(jax.random.uniform(jax.random.fold_in(key, 304), (row_total, 1), jnp.float32, -scale_reach, scale_reach))
    row_scale = row_scale / math.sqrt(math.sinh(2.0 * scale_reach) / (2.0 * scale_reach))
    mixed_rows = math.sqrt(1.0 - common_share) * base_draw + math.sqrt(common_share) * loadings * common_row
    weights = row_scale * mixed_rows / math.sqrt(row_total)
    return weights.astype(jnp.bfloat16)


def with_ends(array, stream_key, smallest, high):
    index_at = [jax.random.randint(jax.random.fold_in(stream_key, axis), (), 0, length) for axis, length in enumerate(array.shape)]
    longest = array.shape.index(max(array.shape))
    neighbour = index_at[:longest] + [(index_at[longest] + 1) % array.shape[longest]] + index_at[longest + 1:]
    return array.at[tuple(index_at)].set(smallest).at[tuple(neighbour)].set(high)


def block_scale(rng, shape, cuts, smallest, high):
    def one(dim, blocks):
        heights = jax.random.uniform(jax.random.fold_in(jax.random.fold_in(rng, 6), dim), (blocks,), jnp.float32, smallest / len(cuts), high / len(cuts))
        return jnp.repeat(jnp.exp(heights), shape[dim] // blocks).reshape((-1,) + (1,) * (len(shape) - dim - 1))

    loudness = one(*cuts[0])
    for cut in cuts[1:]:
        loudness = loudness * one(*cut)
    return loudness


def length_profile(number_of, total, reach, skew):
    portions = [(1 << 20) // math.isqrt(grade ** skew) + 1 for grade in range(2, number_of + 1)]
    spare, given = total - reach - (number_of - 1), [1] * (number_of - 1)
    while spare > 0:
        free = [i for i in range(number_of - 1) if given[i] < reach]
        pool, left = sum([portions[i] for i in free]), spare
        for i in free:
            addition = min(reach - given[i], max(1, left * portions[i] // pool), spare)
            given[i] = given[i] + addition
            spare = spare - addition
    return np.array([reach] + given)


def uneven_parts(stream_key, number_of, total, reach, lean):
    if number_of == 2:
        one = jax.random.randint(stream_key, (), max(1, total - reach), min(reach, total - 1) + 1)
        return jnp.stack([one, total - one])
    tallies = jnp.asarray(length_profile(number_of, total, reach, lean), jnp.int32)
    twos = (number_of - 1) // 2
    source_of, sink = tallies[1:1 + 2 * twos:2], tallies[2:2 + 2 * twos:2]
    slack = jnp.minimum(source_of - 1, reach - sink)
    shifted = jax.random.randint(jax.random.fold_in(stream_key, 1), (twos,), 0, 1 << 20) % (slack + 1)
    tallies = tallies.at[1:1 + 2 * twos:2].set(source_of - shifted).at[2:2 + 2 * twos:2].set(sink + shifted)
    return tallies[jax.random.permutation(jax.random.fold_in(stream_key, 2), number_of)]


def deal_out(own_key, own, number, rows, amount, top, reach, lean):
    sequence = jax.random.permutation(own_key, amount)
    crowded, ordinary = shares(amount, rows * top, reach, lean, True), shares(amount, rows * top, reach, lean, False)
    places = jnp.arange(amount)

    def named(sizes, rotation):
        used = int((sizes > 0).sum())
        fixed = max(1, used // 4)
        moved = fixed + (places - fixed + rotation * (used - fixed)) % max(1, amount - fixed)
        return jnp.zeros((amount,), jnp.int32).at[sequence[jnp.where(places < fixed, places, moved)]].set(jnp.asarray(sizes, jnp.int32))

    sizes = jnp.where(number % 4 == 0, named(crowded, number // 4), named(ordinary, number - number // 4 - 1))
    mixed = jax.random.permutation(jax.random.fold_in(own, 3), amount)
    giver, taker = mixed[0:amount // 2 * 2:2], mixed[1:amount // 2 * 2:2]
    room = jnp.minimum(sizes[giver] - 1, reach - sizes[taker]) // 2
    room = jnp.where((giver == sequence[0]) | (taker == sequence[0]) | (sizes[taker] == 0), 0, jnp.maximum(room, 0))
    moved = jax.random.randint(jax.random.fold_in(own, 4), (amount // 2,), 0, 1 << 20) % (room + 1)
    sizes = sizes.at[giver].add(-moved).at[taker].add(moved)
    members = jnp.searchsorted(jnp.cumsum(sizes), jnp.arange(rows * top), side="right").astype(jnp.int32)
    table = members.reshape(top, rows).T
    table = table[jax.random.permutation(jax.random.fold_in(own, 1), rows)]
    rotation = jax.random.randint(jax.random.fold_in(own, 2), (rows, 1), 0, top)
    return jnp.take_along_axis(table, (jnp.arange(top)[None, :] + rotation) % top, axis=1)


def shares(amount, total, limit, slope, full):
    loads = [(1 << 20) // math.isqrt(grade ** slope) + 1 for grade in range(1, amount + 1)]
    largest = limit if full else min(limit, max(-(-total // amount), total * loads[0] // sum(loads)))
    least = 1 if total - largest >= amount - 1 else 0
    holding, spare = [largest] + [least] * (amount - 1), total - largest - least * (amount - 1)
    while spare > 0:
        candidates = [i for i in range(1, amount) if holding[i] < largest] or [i for i in range(1, amount) if holding[i] < limit]
        pool, remaining = sum([loads[i] for i in candidates]), spare
        for i in candidates:
            addition = min(limit - holding[i], max(1, remaining * loads[i] // pool), spare)
            holding[i] = holding[i] + addition
            spare = spare - addition
    return np.array(holding)


def centred(key, dims, spread, bound, split=(), kind=jnp.bfloat16):
    values = jax.random.normal(key, dims, jnp.float32) * spread
    if len(split) > 0:
        values = block_scale(key, dims, split, -0.22, 0.18) * values
    return jnp.clip(values, min=-bound, max=bound).astype(kind)


def setup_inputs(seed: int = 0, part: int = 0) -> dict:
    splits = jax.random.split(jax.random.key(seed), 12)
    part_keys = jax.random.split(jax.random.fold_in(splits[11], part), 12)
    queries = draw_queries(jax.random.fold_in(jax.random.fold_in(splits[11], part), 71), part)
    new_kv = centred(part_keys[1], (CACHE_SLOTS, REQUESTS, KV_WIDTH), 2.5, 15.0, ((0, 4), (1, 4)))
    kv_pool = draw_kv_pool(jax.random.fold_in(jax.random.fold_in(splits[11], part), 71), part)
    page_counts = jax.vmap(lambda own: uneven_parts(own, REQ_DEV, POOL_DEV, MAX_PAGES, 1))(jax.random.split(part_keys[3], N_BATCH)).reshape((N_BATCH, REQ_DEV)).astype(jnp.int32)
    last_fill = with_ends(jax.random.randint(part_keys[4], (N_BATCH, REQ_DEV), 1, PAGE + 1), jax.random.fold_in(part_keys[4], 1), 1, PAGE).astype(jnp.int32)
    page_order = jax.vmap(lambda own: jax.random.permutation(own, POOL_DEV))(jax.random.split(part_keys[5], N_BATCH)).reshape((N_BATCH, POOL_DEV)).astype(jnp.int32)
    hidden = centred(part_keys[6], (REQUESTS, D), 0.1, 0.59765625, ((0, 4),))
    out_weight = draw_out_weight(jax.random.fold_in(splits[11], 71), part)
    norm_gain = jnp.clip(1.0 + 0.18 * jax.random.normal(splits[8], (D,), jnp.float32), 0.099609375, 1.8984375).astype(jnp.bfloat16)
    sectioned = centred(part_keys[9], (N_HEADS, N_BATCH, SECTION_DEV, PAGE, KV_WIDTH), 1.0, 6.0, ((0, 4), (1, 4)))
    routes_keys = jax.random.split(jax.random.fold_in(part_keys[10], 1), N_HEADS * N_BATCH * SECTION_DEV // SECTION_DEV)
    routes_turns = jax.random.permutation(jax.random.fold_in(part_keys[10], 3), N_HEADS * N_BATCH * SECTION_DEV // SECTION_DEV)
    routes = jax.vmap(lambda own, number: deal_out(jax.random.fold_in(part_keys[10], 2), own, number, SECTION_DEV, KV_HEADS, 1, PER_HEAD_CAP, 2))(routes_keys, routes_turns).reshape((N_HEADS, N_BATCH, SECTION_DEV, 1))
    return {"queries": queries, "new_kv": new_kv, "kv_pool": kv_pool, "page_counts": page_counts, "last_fill": last_fill, "page_order": page_order, "hidden": hidden, "out_weight": out_weight, "norm_gain": norm_gain, "sectioned": sectioned, "routes": routes}


norm_epsilon = 1e-06

def attend(queries, new_kv, kv_pool, counts, fill, order):
    slot_count, pool_pages, page_size, lane_width = kv_pool.shape
    head_dim = lane_width // 2
    requests = queries.shape[0]
    score_scale = 1.0 / head_dim ** 0.5
    position = jnp.arange(pool_pages, dtype=jnp.int32)
    order = order.astype(jnp.int32)
    counts = counts.astype(jnp.int32)
    position_in_order = lax.optimization_barrier(jnp.sum(jnp.where(order[None, :] == position[:, None], position[None, :], 0), axis=1)).astype(jnp.int32)
    count_ends = jnp.cumsum(counts).astype(jnp.int32)
    starts = count_ends - counts
    owner_index = lax.optimization_barrier(jnp.sum((count_ends[None, :] <= position_in_order[:, None]).astype(jnp.int32), axis=1))
    member = owner_index[:, None] == jnp.arange(requests, dtype=jnp.int32)[None, :]
    member_float = member.astype(jnp.float32)
    within = position_in_order - lax.optimization_barrier(jnp.sum(jnp.where(member, starts[None, :], 0), axis=1))
    context = (counts - 1) * page_size + fill.astype(jnp.int32)
    context_limit = lax.optimization_barrier(jnp.sum(jnp.where(member, context[None, :], 0), axis=1))
    live_tokens = within[:, None] * page_size + jnp.arange(page_size, dtype=jnp.int32)[None, :] < context_limit[:, None]
    query_float = queries.astype(jnp.float32)
    page_queries = jnp.einsum('pr,rlgd->lpgd', member_float, query_float, precision=lax.Precision.HIGHEST)
    key_rows = kv_pool[..., :head_dim].astype(jnp.float32)
    value_rows = kv_pool[..., head_dim:].astype(jnp.float32)
    scores = jnp.einsum('lpgd,lptd->lpgt', page_queries, key_rows, precision=lax.Precision.HIGHEST) * score_scale
    scores = jnp.where(live_tokens[None, :, None, :], scores, -1e+30)
    page_top = lax.optimization_barrier(jnp.max(scores, axis=3))
    new_keys = new_kv[..., :head_dim].astype(jnp.float32)
    new_values = new_kv[..., head_dim:].astype(jnp.float32)
    fresh_score = jnp.einsum('rlgd,lrd->lrg', query_float, new_keys, precision=lax.Precision.HIGHEST) * score_scale
    masked_top = jnp.where(member.T[None, :, :, None], page_top[:, None, :, :], -1e+30)
    request_top = jnp.maximum(fresh_score, lax.optimization_barrier(jnp.max(masked_top, axis=2)))
    page_ref = jnp.einsum('pr,lrg->lpg', member_float, request_top, precision=lax.Precision.HIGHEST)
    weight = jnp.where(live_tokens[None, :, None, :], jnp.exp(scores - page_ref[..., None]), 0.0)
    page_den = lax.optimization_barrier(jnp.sum(weight, axis=3))
    weight_rounded = lax.optimization_barrier(weight.astype(jnp.bfloat16)).astype(jnp.float32)
    page_num = jnp.einsum('lpgt,lptd->lpgd', weight_rounded, value_rows, precision=lax.Precision.HIGHEST)
    fresh_weight = jnp.exp(fresh_score - request_top)
    fresh_rounded = lax.optimization_barrier(fresh_weight.astype(jnp.bfloat16)).astype(jnp.float32)
    denominator = jnp.einsum('pr,lpg->lrg', member_float, page_den, precision=lax.Precision.HIGHEST) + fresh_weight
    numerator = jnp.einsum('pr,lpgd->lrgd', member_float, page_num, precision=lax.Precision.HIGHEST)
    numerator = numerator + fresh_rounded[..., None] * new_values[:, :, None, :]
    attended = numerator / denominator[..., None]
    attended = jnp.transpose(attended, (1, 0, 2, 3)).astype(jnp.bfloat16)
    return attended.reshape(requests, -1)

def landing_table(destination, head_total, most_pages):
    sectioned_count = destination.shape[0]
    order_ids = jnp.arange(sectioned_count, dtype=jnp.int32)
    same_head = destination[:, None] == destination[None, :]
    earlier = order_ids[:, None] > order_ids[None, :]
    page_rank = lax.optimization_barrier(jnp.sum((same_head & earlier).astype(jnp.int32), axis=1))
    matches = (destination[None, None, :] == jnp.arange(head_total, dtype=jnp.int32)[:, None, None]) & (page_rank[None, None, :] == jnp.arange(most_pages, dtype=jnp.int32)[None, :, None])
    source_index = lax.optimization_barrier(jnp.sum(jnp.where(matches, order_ids[None, None, :], 0), axis=2)).astype(jnp.int32)
    source_valid = jnp.any(matches, axis=2)
    return (source_index, source_valid)

def reference(queries, new_kv, kv_pool, page_counts, last_fill, page_order, hidden, out_weight, norm_gain, sectioned, routes):
    group_size = Q_HEADS // CACHE_SLOTS
    pieces = []
    for owner_index in range(N_BATCH):
        first_row = owner_index * REQ_DEV
        query_block = queries[first_row:first_row + REQ_DEV].reshape(REQ_DEV, CACHE_SLOTS, group_size, HEAD_DIM)
        pool_block = kv_pool[:, owner_index * POOL_DEV:(owner_index + 1) * POOL_DEV]
        pieces.append(attend(query_block, new_kv[:, first_row:first_row + REQ_DEV], pool_block, page_counts[owner_index], last_fill[owner_index], page_order[owner_index]))
    attn = jnp.concatenate(pieces, axis=0)
    mixed = hidden.astype(jnp.float32) + jnp.dot(attn, out_weight, preferred_element_type=jnp.float32)
    residual_out = mixed.astype(jnp.bfloat16)
    mean_square = lax.optimization_barrier(jnp.mean(mixed * mixed, axis=1, keepdims=True))
    normed = (mixed * lax.rsqrt(mean_square + norm_epsilon) * norm_gain.astype(jnp.float32)).astype(jnp.bfloat16)
    table_fn = jax.vmap(jax.vmap(lambda destination: landing_table(destination, KV_HEADS, PER_HEAD_CAP)))
    source_index, source_valid = table_fn(routes[..., 0].astype(jnp.int32))
    slot_head = jnp.arange(CACHE_SLOTS, dtype=jnp.int32) * KV_HEADS // CACHE_SLOTS
    head_ids = jnp.arange(N_HEADS, dtype=jnp.int32)[None, None, :, None]
    batch_ids = jnp.arange(N_BATCH, dtype=jnp.int32)[None, :, None, None]
    slot_ids = slot_head[:, None, None, None]
    rank_ids = jnp.arange(PER_HEAD_CAP, dtype=jnp.int32)[None, None, None, :]
    chosen = source_index[head_ids, batch_ids, slot_ids, rank_ids]
    present = source_valid[head_ids, batch_ids, slot_ids, rank_ids]
    landed = sectioned[head_ids, batch_ids, chosen]
    arrival = jnp.where(present[..., None, None], landed, jnp.zeros_like(landed)).astype(jnp.bfloat16)
    return (residual_out, normed, arrival)
```

```python
import functools

import jax
import jax.numpy as jnp
from jax import lax
from jax.experimental import pallas as pl
from jax.experimental.pallas import tpu as pltpu
from jax.sharding import PartitionSpec as P

KV_HEADS = 8
MAX_PAGES = 6

norm_epsilon = 1e-06
MESH = pl.DeviceIdType.MESH
CHUNK = 1024
UNROLL = 2


def step_kernel(
    n,
    counts,
    fill,
    order,
    routes,
    queries,
    new_kv,
    kv_pool,
    hidden,
    weight,
    gain,
    sectioned,
    residual_out,
    normed_out,
    arrival,
    sect_v,
    outgoing,
    q_raw,
    q_rows,
    new_raw,
    new_rows,
    kv_v,
    hidden_v,
    gain_v,
    weight_v,
    attn_rows,
    attn_v,
    own_sum,
    terms,
    landed,
    gathered,
    load_sems,
    kv_sems,
    weight_sems,
    own_sems,
    page_send,
    page_recv,
    term_send,
    term_recv,
    block_send,
    block_recv,
):
    me = lax.axis_index("heads")
    slots, pool_pages, page_size, width = kv_v.shape
    head_dim = width // 2
    requests = q_raw.shape[0]
    group = q_rows.shape[2]
    pages = sect_v.shape[0] - 1
    cap = outgoing.shape[2]
    block = terms.shape[2]
    chunk_total, _, chunk = weight_v.shape
    chunks = block // chunk

    def peer(step):
        return lax.rem(me + 1 + step, n)

    def source(step):
        return lax.rem(me + n - 1 - step, n)

    loads = [
        pltpu.make_async_copy(src, dst, load_sems.at[i])
        for i, (src, dst) in enumerate(
            (
                (sectioned.at[0, 0], sect_v.at[pl.ds(0, pages)]),
                (queries, q_raw),
                (new_kv, new_raw),
                (hidden, hidden_v),
                (gain, gain_v),
            )
        )
    ]
    for load in loads[:3]:
        load.start()
    kv_loads = [
        pltpu.make_async_copy(kv_pool.at[l], kv_v.at[l], kv_sems.at[l]) for l in range(slots)
    ]
    for load in kv_loads:
        load.start()

    def weight_load(i):
        column = peer(i // chunks) * block + (i % chunks) * chunk
        return pltpu.make_async_copy(
            weight.at[:, pl.ds(pl.multiple_of(column, chunk), chunk)],
            weight_v.at[i],
            weight_sems.at[i],
        )

    for load in loads[3:]:
        load.start()
    for i in range(chunk_total):
        weight_load(i).start()

    barrier = pltpu.get_barrier_semaphore()
    for step in range(n - 1):
        pl.semaphore_signal(
            barrier, inc=1, device_id={"heads": peer(step)}, device_id_type=MESH
        )

    sect_v[pages] = jnp.zeros(sect_v.shape[1:], sect_v.dtype)
    loads[0].wait()
    page_heads = [routes[0, j] for j in range(pages)]

    def fill_outgoing(step):
        target = peer(step)
        for l in range(slots):
            head = (target * slots + l) * KV_HEADS // (n * slots)
            found = jnp.int32(0)
            picks = [jnp.int32(pages)] * cap
            for j in range(pages):
                hit = page_heads[j] == head
                for k in range(cap):
                    picks[k] = jnp.where(hit & (found == k), j, picks[k])
                found = found + jnp.where(hit, 1, 0)
            for k in range(cap):
                outgoing[step, l, k] = sect_v[picks[k]]

    def page_copy(step, l, place):
        return pltpu.make_async_remote_copy(
            src_ref=outgoing.at[step, l],
            dst_ref=arrival.at[l, 0, place],
            send_sem=page_send.at[step, l],
            recv_sem=page_recv.at[step, l],
            device_id={"heads": peer(step)},
            device_id_type=MESH,
        )

    for step in range(n - 1):
        fill_outgoing(step)
        if step == 0:
            pl.semaphore_wait(barrier, n - 1)
        for l in range(slots):
            page_copy(step, l, me).start()
    fill_outgoing(n - 1)
    own_copies = [
        pltpu.make_async_copy(outgoing.at[n - 1, l], arrival.at[l, 0, me], own_sems.at[l])
        for l in range(slots)
    ]
    for copy in own_copies:
        copy.start()

    loads[1].wait()
    loads[2].wait()
    new_rows[...] = new_raw[...].astype(jnp.float32)
    for l in range(slots):
        for g in range(group):
            first = (l * group + g) * head_dim
            q_rows[l, :, g, :] = q_raw[:, first : first + head_dim].astype(jnp.float32)
    for load in kv_loads:
        load.wait()

    score_scale = 1.0 / head_dim**0.5

    def attend(i, start):
        for sub in range(UNROLL):
            r = i * UNROLL + sub
            count = counts[0, r]
            context = (count - 1) * page_size + fill[0, r]
            picked = [
                order[0, jnp.minimum(start + j, pool_pages - 1)] for j in range(MAX_PAGES)
            ]
            live = (
                lax.broadcasted_iota(jnp.int32, (group, MAX_PAGES * page_size), 1) < context
            )
            for l in range(slots):
                query = q_rows[l, r]
                fresh = new_rows[l, pl.ds(r, 1), :]
                keys = jnp.concatenate([kv_v[l, p, :, :head_dim] for p in picked], axis=0)
                scores = (
                    lax.dot_general(
                        query.astype(jnp.bfloat16),
                        keys,
                        (((1,), (1,)), ((), ())),
                        preferred_element_type=jnp.float32,
                    )
                    * score_scale
                )
                scores = jnp.where(live, scores, -1e30)
                fresh_score = (
                    jnp.sum(query * fresh[:, :head_dim], axis=1, keepdims=True) * score_scale
                )
                top = jnp.maximum(jnp.max(scores, axis=1, keepdims=True), fresh_score)
                w = jnp.where(live, jnp.exp(scores - top), 0.0)
                fresh_w = jnp.exp(fresh_score - top)
                den = jnp.sum(w, axis=1, keepdims=True) + fresh_w
                values = jnp.concatenate([kv_v[l, p, :, head_dim:] for p in picked], axis=0)
                num = jnp.dot(w.astype(jnp.bfloat16), values, preferred_element_type=jnp.float32)
                num = num + fresh_w.astype(jnp.bfloat16).astype(jnp.float32) * fresh[:, head_dim:]
                attn_rows[l, r] = num / den
            start = start + count
        return start

    lax.fori_loop(0, requests // UNROLL, attend, jnp.int32(0))
    for l in range(slots):
        for g in range(group):
            first = (l * group + g) * head_dim
            attn_v[:, first : first + head_dim] = attn_rows[l, :, g, :].astype(jnp.bfloat16)

    def term_copy(step):
        return pltpu.make_async_remote_copy(
            src_ref=terms.at[step],
            dst_ref=landed.at[step],
            send_sem=term_send.at[step],
            recv_sem=term_recv.at[step],
            device_id={"heads": peer(step)},
            device_id_type=MESH,
        )

    def project(step, carry):
        for part in range(chunks):
            i = step * chunks + part
            weight_load(i).wait()
            term = jnp.dot(attn_v[...], weight_v[i], preferred_element_type=jnp.float32)
            own_sum[:, part * chunk : (part + 1) * chunk] = term
            terms[step, :, part * chunk : (part + 1) * chunk] = term.astype(jnp.bfloat16)

        @pl.when(step < n - 1)
        def _():
            term_copy(step).start()

        return carry

    lax.fori_loop(0, n, project, 0)
    loads[3].wait()
    loads[4].wait()

    column = pl.multiple_of(me * block, block)
    total = own_sum[...] + hidden_v[:, pl.ds(column, block)].astype(jnp.float32)
    for step in range(n - 1):
        term_copy(step).wait_recv()
        total = total + landed[step].astype(jnp.float32)
    gathered[me] = total.astype(jnp.bfloat16)

    def block_copy(step, place):
        return pltpu.make_async_remote_copy(
            src_ref=gathered.at[place],
            dst_ref=gathered.at[place],
            send_sem=block_send.at[step],
            recv_sem=block_recv.at[step],
            device_id={"heads": peer(step)},
            device_id_type=MESH,
        )

    for step in range(n - 1):
        block_copy(step, me).start()
    for step in range(n - 1):
        term_copy(step).wait_send()
    for step in range(n - 1):
        block_copy(step, source(step)).wait_recv()
    square = jnp.zeros((requests, 1), jnp.float32)
    for c in range(n):
        mixed = gathered[c].astype(jnp.float32)
        square = square + jnp.sum(mixed * mixed, axis=1, keepdims=True)
    factor = lax.rsqrt(square / (n * block) + norm_epsilon)
    for c in range(n):
        piece = gathered[c]
        here = slice(c * block, (c + 1) * block)
        residual_out[:, here] = piece
        normed_out[:, here] = (
            piece.astype(jnp.float32) * factor * gain_v[:, here].astype(jnp.float32)
        ).astype(jnp.bfloat16)

    for step in range(n - 1):
        block_copy(step, me).wait_send()
        for l in range(slots):
            page_copy(step, l, me).wait_send()
            page_copy(step, l, source(step)).wait_recv()
    for copy in own_copies:
        copy.wait()


def per_device(
    queries,
    new_kv,
    kv_pool,
    page_counts,
    last_fill,
    page_order,
    hidden,
    out_weight,
    norm_gain,
    sectioned,
    routes,
    *,
    cap,
):
    n = lax.axis_size("heads")
    slots, pool_pages, page_size, width = kv_pool.shape
    head_dim = width // 2
    requests, model = hidden.shape
    rows = out_weight.shape[0]
    group = rows // (slots * head_dim)
    pages = sectioned.shape[2]
    block = model // n
    chunk = min(CHUNK, block)
    bf16, f32 = jnp.bfloat16, jnp.float32
    dma = pltpu.SemaphoreType.DMA
    smem = pl.BlockSpec(memory_space=pltpu.SMEM)
    hbm = pl.BlockSpec(memory_space=pl.ANY)
    vmem = pl.BlockSpec(memory_space=pltpu.VMEM)
    return pl.pallas_call(
        functools.partial(step_kernel, n),
        out_shape=(
            jax.ShapeDtypeStruct((requests, model), bf16),
            jax.ShapeDtypeStruct((requests, model), bf16),
            jax.ShapeDtypeStruct((slots, 1, n, cap, page_size, width), bf16),
        ),
        in_specs=[smem] * 4 + [hbm] * 7,
        out_specs=(vmem, vmem, hbm),
        scratch_shapes=[
            pltpu.VMEM((pages + 1, page_size, width), bf16),
            pltpu.VMEM((n, slots, cap, page_size, width), bf16),
            pltpu.VMEM((requests, rows), bf16),
            pltpu.VMEM((slots, requests, group, head_dim), f32),
            pltpu.VMEM((slots, requests, width), bf16),
            pltpu.VMEM((slots, requests, width), f32),
            pltpu.VMEM((slots, pool_pages, page_size, width), bf16),
            pltpu.VMEM((requests, model), bf16),
            pltpu.VMEM((1, model), bf16),
            pltpu.VMEM((model // chunk, rows, chunk), bf16),
            pltpu.VMEM((slots, requests, group, head_dim), f32),
            pltpu.VMEM((requests, rows), bf16),
            pltpu.VMEM((requests, block), f32),
            pltpu.VMEM((n, requests, block), bf16),
            pltpu.VMEM((n - 1, requests, block), bf16),
            pltpu.VMEM((n, requests, block), bf16),
            dma((5,)),
            dma((slots,)),
            dma((model // chunk,)),
            dma((slots,)),
            dma((n - 1, slots)),
            dma((n - 1, slots)),
            dma((n - 1,)),
            dma((n - 1,)),
            dma((n - 1,)),
            dma((n - 1,)),
        ],
        compiler_params=pltpu.CompilerParams(
            collective_id=0, has_side_effects=True, vmem_limit_bytes=60 * 1024 * 1024
        ),
        name="decode_step",
    )(
        page_counts,
        last_fill,
        page_order,
        routes.reshape(1, pages),
        queries,
        new_kv,
        kv_pool,
        hidden,
        out_weight,
        norm_gain.reshape(1, model),
        sectioned,
    )


PER_HEAD_CAP = 2


def solution(mesh):
    return jax.shard_map(
        functools.partial(per_device, cap=PER_HEAD_CAP),
        mesh=mesh,
        in_specs=(
            P(("groups", "batch"), "heads"),
            P(("groups", "heads"), "batch", None),
            P(("groups", "heads"), "batch", None, None),
            P(("groups", "batch"), None),
            P(("groups", "batch"), None),
            P(("groups", "batch"), None),
            P(("groups", "batch"), None),
            P("heads", None),
            P(),
            P(("groups", "heads"), "batch", None, None, None),
            P(("groups", "heads"), "batch", None, None),
        ),
        out_specs=(
            P(("groups", "batch"), None),
            P(("groups", "batch"), None),
            P(("groups", "heads"), "batch", None, None, None, None),
        ),
        check_vma=False,
    )
```

```python
import functools

import jax
import jax.numpy as jnp
from jax import lax
from jax.experimental import pallas as pl
from jax.experimental.pallas import tpu as pltpu
from jax.sharding import PartitionSpec as P

KV_HEADS = 8
MAX_PAGES = 6

norm_epsilon = 1e-06
MESH = pl.DeviceIdType.MESH
CHUNK = 1024
UNROLL = 4
FIRST_PAGES = 5


def step_kernel(
    n,
    counts,
    fill,
    order,
    routes,
    queries,
    new_kv,
    kv_pool,
    hidden,
    weight,
    sectioned,
    gathered,
    arrival,
    sect_v,
    outgoing,
    q_raw,
    q_rows,
    new_raw,
    new_rows,
    kv_v,
    hidden_v,
    weight_v,
    attn_rows,
    attn_v,
    terms,
    landed,
    load_sems,
    kv_sems,
    weight_sems,
    own_sems,
    page_send,
    page_recv,
    term_send,
    term_recv,
    block_send,
    block_recv,
):
    me = lax.axis_index("heads")
    slots, pool_pages, page_size, width = kv_v.shape
    head_dim = width // 2
    requests = q_raw.shape[0]
    group = q_rows.shape[2]
    pages = sect_v.shape[0] - 1
    cap = outgoing.shape[2]
    block = terms.shape[2]
    chunk_total, _, chunk = weight_v.shape
    chunks = block // chunk

    bits = [1 << s for s in range(n.bit_length() - 1)]

    def partner(mask):
        place = me
        for bit in bits:
            if mask & bit:
                place = place + bit * (1 - 2 * lax.rem(me // bit, 2))
        return place

    def lowest(mask):
        return mask & -mask if mask else n

    masks = sorted(range(n), key=lambda mask: (lowest(mask), -mask))
    far = [mask for mask in range(n - 1, 0, -1) if mask & (n // 2)]
    near = [mask for mask in range(n - 1, 0, -1) if not mask & (n // 2)]

    loads = [
        pltpu.make_async_copy(src, dst, load_sems.at[i])
        for i, (src, dst) in enumerate(
            (
                (sectioned.at[0, 0], sect_v.at[pl.ds(0, pages)]),
                (queries, q_raw),
                (new_kv, new_raw),
                (hidden, hidden_v),
            )
        )
    ]
    for load in loads[:3]:
        load.start()
    kv_loads = [
        pltpu.make_async_copy(kv_pool.at[l], kv_v.at[l], kv_sems.at[l]) for l in range(slots)
    ]
    for load in kv_loads:
        load.start()

    def weight_load(i):
        column = partner(masks[i // chunks]) * block + (i % chunks) * chunk
        return pltpu.make_async_copy(
            weight.at[:, pl.ds(pl.multiple_of(column, chunk), chunk)],
            weight_v.at[i],
            weight_sems.at[i],
        )

    for load in loads[3:]:
        load.start()
    for i in range(chunk_total):
        weight_load(i).start()

    barrier = pltpu.get_barrier_semaphore()
    for mask in range(1, n):
        pl.semaphore_signal(
            barrier, inc=1, device_id={"heads": partner(mask)}, device_id_type=MESH
        )

    sect_v[pages] = jnp.zeros(sect_v.shape[1:], sect_v.dtype)
    loads[0].wait()
    page_heads = [routes[0, j] for j in range(pages)]

    def fill_outgoing(mask, l):
        head = (partner(mask) * slots + l) * KV_HEADS // (n * slots)
        found = jnp.int32(0)
        picks = [jnp.int32(pages)] * cap
        for j in range(pages):
            hit = page_heads[j] == head
            for k in range(cap):
                picks[k] = jnp.where(hit & (found == k), j, picks[k])
            found = found + jnp.where(hit, 1, 0)
        for k in range(cap):
            outgoing[mask, l, k] = sect_v[picks[k]]

    def page_copy(mask, l, k, place):
        return pltpu.make_async_remote_copy(
            src_ref=outgoing.at[mask, l, k],
            dst_ref=arrival.at[l, 0, place, k],
            send_sem=page_send.at[mask, l, k],
            recv_sem=page_recv.at[mask, l, k],
            device_id={"heads": partner(mask)},
            device_id_type=MESH,
        )

    far_pages = [(mask, l, k) for l in range(slots) for mask in far for k in range(cap)]
    first_count = len(far_pages) * FIRST_PAGES // 8
    waiting = far_pages[first_count:]

    def send_waiting(count):
        for spot in waiting[:count]:
            page_copy(*spot, me).start()
        del waiting[:count]

    filled = set()
    for spot in far_pages[:first_count]:
        if spot[:2] not in filled:
            filled.add(spot[:2])
            fill_outgoing(*spot[:2])
        if len(filled) == 1 and spot == far_pages[0]:
            pl.semaphore_wait(barrier, n - 1)
        page_copy(*spot, me).start()
    for mask in near:
        for l in range(slots):
            fill_outgoing(mask, l)
            for k in range(cap):
                page_copy(mask, l, k, me).start()
    for mask in [*far, 0]:
        for l in range(slots):
            if (mask, l) not in filled:
                fill_outgoing(mask, l)
    own_copies = [
        pltpu.make_async_copy(outgoing.at[0, l], arrival.at[l, 0, me], own_sems.at[l])
        for l in range(slots)
    ]
    for copy in own_copies:
        copy.start()

    loads[1].wait()
    loads[2].wait()
    new_rows[...] = new_raw[...].astype(jnp.float32)
    for l in range(slots):
        for g in range(group):
            first = (l * group + g) * head_dim
            q_rows[l, :, g, :] = q_raw[:, first : first + head_dim].astype(jnp.float32)
    for load in kv_loads:
        load.wait()

    score_scale = 1.0 / head_dim**0.5

    def attend(i, start):
        chains = []
        for sub in range(UNROLL):
            r = i * UNROLL + sub
            count = counts[0, r]
            context = (count - 1) * page_size + fill[0, r]
            picked = [
                order[0, jnp.minimum(start + j, pool_pages - 1)] for j in range(MAX_PAGES)
            ]
            start = start + count
            chains += [(l, r, context, picked) for l in range(slots)]
        shape = (group, MAX_PAGES * page_size)
        token = lax.broadcasted_iota(jnp.int32, shape, 1)
        raw = []
        for l, r, context, picked in chains:
            keys = jnp.concatenate([kv_v[l, p, :, :head_dim] for p in picked], axis=0)
            raw.append(
                lax.dot_general(
                    q_rows[l, r].astype(jnp.bfloat16),
                    keys,
                    (((1,), (1,)), ((), ())),
                    preferred_element_type=jnp.float32,
                )
            )
        fresh_scores = [
            jnp.sum(q_rows[l, r] * new_rows[l, pl.ds(r, 1), :][:, :head_dim], axis=1, keepdims=True)
            * score_scale
            for l, r, context, picked in chains
        ]
        scores = [
            jnp.where(token < chain[2], value * score_scale, -1e30)
            for chain, value in zip(chains, raw)
        ]
        tops = [
            jnp.maximum(jnp.max(value, axis=1, keepdims=True), fresh)
            for value, fresh in zip(scores, fresh_scores)
        ]
        ws = [
            jnp.where(token < chain[2], jnp.exp(value - top), 0.0)
            for chain, value, top in zip(chains, scores, tops)
        ]
        fresh_ws = [jnp.exp(fresh - top) for fresh, top in zip(fresh_scores, tops)]
        nums = []
        for (l, r, context, picked), w in zip(chains, ws):
            values = jnp.concatenate([kv_v[l, p, :, head_dim:] for p in picked], axis=0)
            nums.append(
                jnp.dot(w.astype(jnp.bfloat16), values, preferred_element_type=jnp.float32)
            )
        dens = [
            jnp.sum(w, axis=1, keepdims=True) + fresh for w, fresh in zip(ws, fresh_ws)
        ]
        for (l, r, context, picked), num, den, fresh in zip(chains, nums, dens, fresh_ws):
            rounded = fresh.astype(jnp.bfloat16).astype(jnp.float32)
            num = num + rounded * new_rows[l, pl.ds(r, 1), :][:, head_dim:]
            attn_rows[l, r] = num / den
        return start

    lax.fori_loop(0, requests // UNROLL, attend, jnp.int32(0))
    for l in range(slots):
        for g in range(group):
            first = (l * group + g) * head_dim
            attn_v[:, first : first + head_dim] = attn_rows[l, :, g, :].astype(jnp.bfloat16)

    def term_copy(mask):
        return pltpu.make_async_remote_copy(
            src_ref=terms.at[mask],
            dst_ref=landed.at[mask],
            send_sem=term_send.at[mask],
            recv_sem=term_recv.at[mask],
            device_id={"heads": partner(lowest(mask))},
            device_id_type=MESH,
        )

    def block_copy(mask, place):
        return pltpu.make_async_remote_copy(
            src_ref=gathered.at[place],
            dst_ref=gathered.at[place],
            send_sem=block_send.at[mask],
            recv_sem=block_recv.at[mask],
            device_id={"heads": partner(lowest(mask))},
            device_id_type=MESH,
        )

    quarter = -(-len(waiting) // 3)
    for i, mask in enumerate(masks):
        parts = []
        for part in range(chunks):
            weight_load(i * chunks + part).wait()
            parts.append(
                jnp.dot(
                    attn_v[...], weight_v[i * chunks + part], preferred_element_type=jnp.float32
                )
            )
        total = parts[0] if chunks == 1 else jnp.concatenate(parts, axis=1)
        if mask == 0:
            loads[3].wait()
            column = pl.multiple_of(me * block, block)
            total = total + hidden_v[:, pl.ds(column, block)].astype(jnp.float32)
        for bit in bits:
            if bit < lowest(mask):
                term_copy(mask + bit).wait_recv()
                total = total + landed[mask + bit].astype(jnp.float32)
        if mask:
            terms[mask] = total.astype(jnp.bfloat16)
            term_copy(mask).start()
            if i == n - 2:
                send_waiting(quarter)
        else:
            gathered[me] = total.astype(jnp.bfloat16)

    for bit in reversed(bits):
        block_copy(bit, me).start()
        if bit == bits[-1]:
            send_waiting(quarter)
    for bit in reversed(bits):
        for mask in range(1, n):
            if lowest(mask) == bit:
                block_copy(mask, partner(mask)).wait_recv()
                for lower in bits:
                    if lower < bit:
                        block_copy(mask + lower, partner(mask)).start()
        if bit == bits[-1]:
            send_waiting(len(waiting))

    for mask in range(1, n):
        term_copy(mask).wait_send()
        block_copy(mask, me).wait_send()
        for l in range(slots):
            for k in range(cap):
                page_copy(mask, l, k, me).wait_send()
                page_copy(mask, l, k, partner(mask)).wait_recv()
    for copy in own_copies:
        copy.wait()


def finish_kernel(gathered, gain, landed, residual_out, normed_out, arrival, held, sems):
    n, requests, block = gathered.shape
    slots = held.shape[0]
    into = [pltpu.make_async_copy(landed.at[l], held.at[l], sems.at[0, l]) for l in range(slots)]
    out = [pltpu.make_async_copy(held.at[l], arrival.at[l], sems.at[1, l]) for l in range(slots)]
    for copy in into:
        copy.start()
    square = jnp.zeros((requests, 1), jnp.float32)
    for c in range(n):
        mixed = gathered[c].astype(jnp.float32)
        square = square + jnp.sum(mixed * mixed, axis=1, keepdims=True)
    factor = lax.rsqrt(square / (n * block) + norm_epsilon)
    for l in range(slots):
        into[l].wait()
        out[l].start()
    for c in range(n):
        piece = gathered[c]
        here = slice(c * block, (c + 1) * block)
        residual_out[:, here] = piece
        scale = gain[here].astype(jnp.float32).reshape(1, block)
        normed_out[:, here] = (piece.astype(jnp.float32) * factor * scale).astype(jnp.bfloat16)
    for copy in out:
        copy.wait()


def per_device(
    queries,
    new_kv,
    kv_pool,
    page_counts,
    last_fill,
    page_order,
    hidden,
    out_weight,
    norm_gain,
    sectioned,
    routes,
    *,
    cap,
):
    n = lax.axis_size("heads")
    slots, pool_pages, page_size, width = kv_pool.shape
    head_dim = width // 2
    requests, model = hidden.shape
    rows = out_weight.shape[0]
    group = rows // (slots * head_dim)
    pages = sectioned.shape[2]
    block = model // n
    chunk = min(CHUNK, block)
    bf16, f32 = jnp.bfloat16, jnp.float32
    dma = pltpu.SemaphoreType.DMA
    smem = pl.BlockSpec(memory_space=pltpu.SMEM)
    hbm = pl.BlockSpec(memory_space=pl.ANY)
    vmem = pl.BlockSpec(memory_space=pltpu.VMEM)
    landing = jax.ShapeDtypeStruct((slots, 1, n, cap, page_size, width), bf16)
    gathered, landed = pl.pallas_call(
        functools.partial(step_kernel, n),
        out_shape=(jax.ShapeDtypeStruct((n, requests, block), bf16), landing),
        in_specs=[smem] * 4 + [hbm] * 6,
        out_specs=(vmem, hbm),
        scratch_shapes=[
            pltpu.VMEM((pages + 1, page_size, width), bf16),
            pltpu.VMEM((n, slots, cap, page_size, width), bf16),
            pltpu.VMEM((requests, rows), bf16),
            pltpu.VMEM((slots, requests, group, head_dim), f32),
            pltpu.VMEM((slots, requests, width), bf16),
            pltpu.VMEM((slots, requests, width), f32),
            pltpu.VMEM((slots, pool_pages, page_size, width), bf16),
            pltpu.VMEM((requests, model), bf16),
            pltpu.VMEM((model // chunk, rows, chunk), bf16),
            pltpu.VMEM((slots, requests, group, head_dim), f32),
            pltpu.VMEM((requests, rows), bf16),
            pltpu.VMEM((n, requests, block), bf16),
            pltpu.VMEM((n, requests, block), bf16),
            dma((4,)),
            dma((slots,)),
            dma((model // chunk,)),
            dma((slots,)),
            dma((n, slots, cap)),
            dma((n, slots, cap)),
            dma((n,)),
            dma((n,)),
            dma((n,)),
            dma((n,)),
        ],
        compiler_params=pltpu.CompilerParams(
            collective_id=0, has_side_effects=True, vmem_limit_bytes=60 * 1024 * 1024
        ),
        name="decode_step",
    )(
        page_counts,
        last_fill,
        page_order,
        routes.reshape(1, pages),
        queries,
        new_kv,
        kv_pool,
        hidden,
        out_weight,
        sectioned,
    )
    return pl.pallas_call(
        finish_kernel,
        out_shape=(
            jax.ShapeDtypeStruct((requests, model), bf16),
            jax.ShapeDtypeStruct((requests, model), bf16),
            landing,
        ),
        in_specs=[vmem, vmem, hbm],
        out_specs=(vmem, vmem, hbm),
        scratch_shapes=[pltpu.VMEM(landing.shape, bf16), dma((2, slots))],
        name="finish",
    )(gathered, norm_gain, landed)


PER_HEAD_CAP = 2


def solution(mesh):
    return jax.shard_map(
        functools.partial(per_device, cap=PER_HEAD_CAP),
        mesh=mesh,
        in_specs=(
            P(("groups", "batch"), "heads"),
            P(("groups", "heads"), "batch", None),
            P(("groups", "heads"), "batch", None, None),
            P(("groups", "batch"), None),
            P(("groups", "batch"), None),
            P(("groups", "batch"), None),
            P(("groups", "batch"), None),
            P("heads", None),
            P(),
            P(("groups", "heads"), "batch", None, None, None),
            P(("groups", "heads"), "batch", None, None),
        ),
        out_specs=(
            P(("groups", "batch"), None),
            P(("groups", "batch"), None),
            P(("groups", "heads"), "batch", None, None, None, None),
        ),
        check_vma=False,
    )
```

```python
import functools

import jax
import jax.numpy as jnp
from jax import lax
from jax.experimental import pallas as pl
from jax.experimental.pallas import tpu as pltpu
from jax.sharding import PartitionSpec as P

KV_HEADS = 8
MAX_PAGES = 6

norm_epsilon = 1e-06
MESH = pl.DeviceIdType.MESH
CHUNK = 1024
UNROLL = 4
FIRST_PAGES = 5


def step_kernel(
    n,
    counts,
    fill,
    order,
    routes,
    queries,
    new_kv,
    kv_pool,
    hidden,
    weight,
    sectioned,
    gathered,
    arrival,
    sect_v,
    outgoing,
    q_raw,
    q_rows,
    new_raw,
    new_rows,
    kv_v,
    hidden_v,
    weight_v,
    attn_rows,
    attn_v,
    terms,
    landed,
    load_sems,
    kv_sems,
    weight_sems,
    own_sems,
    page_send,
    page_recv,
    term_send,
    term_recv,
    block_send,
    block_recv,
):
    me = lax.axis_index("heads")
    slots, pool_pages, page_size, width = kv_v.shape
    head_dim = width // 2
    requests = q_raw.shape[0]
    group = q_rows.shape[2]
    pages = sect_v.shape[0] - 1
    cap = outgoing.shape[2]
    block = terms.shape[2]
    chunk_total, _, chunk = weight_v.shape
    chunks = block // chunk

    bits = [1 << s for s in range(n.bit_length() - 1)]

    def partner(mask):
        place = me
        for bit in bits:
            if mask & bit:
                place = place + bit * (1 - 2 * lax.rem(me // bit, 2))
        return place

    def lowest(mask):
        return mask & -mask if mask else n

    masks = sorted(range(n), key=lambda mask: (lowest(mask), -mask))
    far = [mask for mask in range(n - 1, 0, -1) if mask & (n // 2)]
    near = [mask for mask in range(n - 1, 0, -1) if not mask & (n // 2)]

    loads = [
        pltpu.make_async_copy(src, dst, load_sems.at[i])
        for i, (src, dst) in enumerate(
            (
                (sectioned.at[0, 0], sect_v.at[pl.ds(0, pages)]),
                (queries, q_raw),
                (new_kv, new_raw),
                (hidden, hidden_v),
            )
        )
    ]
    for load in loads[:3]:
        load.start()
    kv_loads = [
        pltpu.make_async_copy(kv_pool.at[l], kv_v.at[l], kv_sems.at[l]) for l in range(slots)
    ]
    for load in kv_loads:
        load.start()

    def weight_load(i):
        column = partner(masks[i // chunks]) * block + (i % chunks) * chunk
        return pltpu.make_async_copy(
            weight.at[:, pl.ds(pl.multiple_of(column, chunk), chunk)],
            weight_v.at[i],
            weight_sems.at[i],
        )

    for load in loads[3:]:
        load.start()
    for i in range(chunk_total):
        weight_load(i).start()

    barrier = pltpu.get_barrier_semaphore()
    for mask in range(1, n):
        pl.semaphore_signal(
            barrier, inc=1, device_id={"heads": partner(mask)}, device_id_type=MESH
        )

    sect_v[pages] = jnp.zeros(sect_v.shape[1:], sect_v.dtype)
    loads[0].wait()
    page_heads = [routes[0, j] for j in range(pages)]

    def fill_outgoing(mask, l):
        head = (partner(mask) * slots + l) * KV_HEADS // (n * slots)
        found = jnp.int32(0)
        picks = [jnp.int32(pages)] * cap
        for j in range(pages):
            hit = page_heads[j] == head
            for k in range(cap):
                picks[k] = jnp.where(hit & (found == k), j, picks[k])
            found = found + jnp.where(hit, 1, 0)
        for k in range(cap):
            outgoing[mask, l, k] = sect_v[picks[k]]

    def page_copy(mask, l, k, place):
        return pltpu.make_async_remote_copy(
            src_ref=outgoing.at[mask, l, k],
            dst_ref=arrival.at[l, 0, place, k],
            send_sem=page_send.at[mask, l, k],
            recv_sem=page_recv.at[mask, l, k],
            device_id={"heads": partner(mask)},
            device_id_type=MESH,
        )

    far_pages = [(mask, l, k) for l in range(slots) for mask in far for k in range(cap)]
    first_count = len(far_pages) * FIRST_PAGES // 8
    waiting = far_pages[first_count:]

    def send_waiting(count):
        for spot in waiting[:count]:
            page_copy(*spot, me).start()
        del waiting[:count]

    for i, mask in enumerate(near):
        for l in range(slots):
            fill_outgoing(mask, l)
            if i == 0 and l == 0:
                pl.semaphore_wait(barrier, n - 1)
            for k in range(cap):
                page_copy(mask, l, k, me).start()
    filled = set()
    for spot in far_pages[:first_count]:
        if spot[:2] not in filled:
            filled.add(spot[:2])
            fill_outgoing(*spot[:2])
        page_copy(*spot, me).start()
    for mask in [*far, 0]:
        for l in range(slots):
            if (mask, l) not in filled:
                fill_outgoing(mask, l)
    own_copies = [
        pltpu.make_async_copy(outgoing.at[0, l], arrival.at[l, 0, me], own_sems.at[l])
        for l in range(slots)
    ]
    for copy in own_copies:
        copy.start()

    loads[1].wait()
    loads[2].wait()
    new_rows[...] = new_raw[...].astype(jnp.float32)
    for l in range(slots):
        for g in range(group):
            first = (l * group + g) * head_dim
            q_rows[l, :, g, :] = q_raw[:, first : first + head_dim].astype(jnp.float32)
    for load in kv_loads:
        load.wait()

    score_scale = 1.0 / head_dim**0.5

    def attend(i, start):
        chains = []
        for sub in range(UNROLL):
            r = i * UNROLL + sub
            count = counts[0, r]
            context = (count - 1) * page_size + fill[0, r]
            picked = [
                order[0, jnp.minimum(start + j, pool_pages - 1)] for j in range(MAX_PAGES)
            ]
            start = start + count
            chains += [(l, r, context, picked) for l in range(slots)]
        shape = (group, MAX_PAGES * page_size)
        token = lax.broadcasted_iota(jnp.int32, shape, 1)
        raw = []
        for l, r, context, picked in chains:
            keys = jnp.concatenate([kv_v[l, p, :, :head_dim] for p in picked], axis=0)
            raw.append(
                lax.dot_general(
                    q_rows[l, r].astype(jnp.bfloat16),
                    keys,
                    (((1,), (1,)), ((), ())),
                    preferred_element_type=jnp.float32,
                )
            )
        fresh_scores = [
            jnp.sum(q_rows[l, r] * new_rows[l, pl.ds(r, 1), :][:, :head_dim], axis=1, keepdims=True)
            * score_scale
            for l, r, context, picked in chains
        ]
        scores = [
            jnp.where(token < chain[2], value * score_scale, -1e30)
            for chain, value in zip(chains, raw)
        ]
        tops = [
            jnp.maximum(jnp.max(value, axis=1, keepdims=True), fresh)
            for value, fresh in zip(scores, fresh_scores)
        ]
        ws = [
            jnp.where(token < chain[2], jnp.exp(value - top), 0.0)
            for chain, value, top in zip(chains, scores, tops)
        ]
        fresh_ws = [jnp.exp(fresh - top) for fresh, top in zip(fresh_scores, tops)]
        nums = []
        for (l, r, context, picked), w in zip(chains, ws):
            values = jnp.concatenate([kv_v[l, p, :, head_dim:] for p in picked], axis=0)
            nums.append(
                jnp.dot(w.astype(jnp.bfloat16), values, preferred_element_type=jnp.float32)
            )
        dens = [
            jnp.sum(w, axis=1, keepdims=True) + fresh for w, fresh in zip(ws, fresh_ws)
        ]
        for (l, r, context, picked), num, den, fresh in zip(chains, nums, dens, fresh_ws):
            rounded = fresh.astype(jnp.bfloat16).astype(jnp.float32)
            num = num + rounded * new_rows[l, pl.ds(r, 1), :][:, head_dim:]
            attn_rows[l, r] = num / den
        return start

    lax.fori_loop(0, requests // UNROLL, attend, jnp.int32(0))
    for l in range(slots):
        for g in range(group):
            first = (l * group + g) * head_dim
            attn_v[:, first : first + head_dim] = attn_rows[l, :, g, :].astype(jnp.bfloat16)

    def term_copy(mask):
        return pltpu.make_async_remote_copy(
            src_ref=terms.at[mask],
            dst_ref=landed.at[mask],
            send_sem=term_send.at[mask],
            recv_sem=term_recv.at[mask],
            device_id={"heads": partner(lowest(mask))},
            device_id_type=MESH,
        )

    def block_copy(mask, place):
        return pltpu.make_async_remote_copy(
            src_ref=gathered.at[place],
            dst_ref=gathered.at[place],
            send_sem=block_send.at[mask],
            recv_sem=block_recv.at[mask],
            device_id={"heads": partner(lowest(mask))},
            device_id_type=MESH,
        )

    quarter = -(-len(waiting) // 3)
    for i, mask in enumerate(masks):
        parts = []
        for part in range(chunks):
            weight_load(i * chunks + part).wait()
            parts.append(
                jnp.dot(
                    attn_v[...], weight_v[i * chunks + part], preferred_element_type=jnp.float32
                )
            )
        total = parts[0] if chunks == 1 else jnp.concatenate(parts, axis=1)
        if mask == 0:
            loads[3].wait()
            column = pl.multiple_of(me * block, block)
            total = total + hidden_v[:, pl.ds(column, block)].astype(jnp.float32)
        for bit in bits:
            if bit < lowest(mask):
                term_copy(mask + bit).wait_recv()
                total = total + landed[mask + bit].astype(jnp.float32)
        if mask:
            terms[mask] = total.astype(jnp.bfloat16)
            term_copy(mask).start()
            if i == n - 2:
                send_waiting(quarter)
        else:
            gathered[me] = total.astype(jnp.bfloat16)

    for bit in reversed(bits):
        block_copy(bit, me).start()
        if bit == bits[-1]:
            send_waiting(quarter)
    for bit in reversed(bits):
        for mask in range(1, n):
            if lowest(mask) == bit:
                block_copy(mask, partner(mask)).wait_recv()
                for lower in bits:
                    if lower < bit:
                        block_copy(mask + lower, partner(mask)).start()
        if bit == bits[-1]:
            send_waiting(len(waiting))

    for mask in range(1, n):
        term_copy(mask).wait_send()
        block_copy(mask, me).wait_send()
        for l in range(slots):
            for k in range(cap):
                page_copy(mask, l, k, me).wait_send()
                page_copy(mask, l, k, partner(mask)).wait_recv()
    for copy in own_copies:
        copy.wait()


def finish_kernel(
    gathered_in, gain_in, landed, residual_out, normed_out, arrival, held, gathered, gain, sems, in_sems
):
    n, requests, block = gathered.shape
    loads = [
        pltpu.make_async_copy(gathered_in, gathered, in_sems.at[0]),
        pltpu.make_async_copy(gain_in, gain, in_sems.at[1]),
    ]
    for load in loads:
        load.start()
    slots = held.shape[0]
    into = [pltpu.make_async_copy(landed.at[l], held.at[l], sems.at[0, l]) for l in range(slots)]
    out = [pltpu.make_async_copy(held.at[l], arrival.at[l], sems.at[1, l]) for l in range(slots)]
    for copy in into:
        copy.start()
    for load in loads:
        load.wait()
    square = jnp.zeros((requests, 1), jnp.float32)
    for c in range(n):
        mixed = gathered[c].astype(jnp.float32)
        square = square + jnp.sum(mixed * mixed, axis=1, keepdims=True)
    factor = lax.rsqrt(square / (n * block) + norm_epsilon)
    for l in range(slots):
        into[l].wait()
        out[l].start()
    for c in range(n):
        piece = gathered[c]
        here = slice(c * block, (c + 1) * block)
        residual_out[:, here] = piece
        scale = gain[here].astype(jnp.float32).reshape(1, block)
        normed_out[:, here] = (piece.astype(jnp.float32) * factor * scale).astype(jnp.bfloat16)
    for copy in out:
        copy.wait()


def per_device(
    queries,
    new_kv,
    kv_pool,
    page_counts,
    last_fill,
    page_order,
    hidden,
    out_weight,
    norm_gain,
    sectioned,
    routes,
    *,
    cap,
):
    n = lax.axis_size("heads")
    slots, pool_pages, page_size, width = kv_pool.shape
    head_dim = width // 2
    requests, model = hidden.shape
    rows = out_weight.shape[0]
    group = rows // (slots * head_dim)
    pages = sectioned.shape[2]
    block = model // n
    chunk = min(CHUNK, block)
    bf16, f32 = jnp.bfloat16, jnp.float32
    dma = pltpu.SemaphoreType.DMA
    smem = pl.BlockSpec(memory_space=pltpu.SMEM)
    hbm = pl.BlockSpec(memory_space=pl.ANY)
    vmem = pl.BlockSpec(memory_space=pltpu.VMEM)
    landing = jax.ShapeDtypeStruct((slots, 1, n, cap, page_size, width), bf16)
    gathered, landed = pl.pallas_call(
        functools.partial(step_kernel, n),
        out_shape=(jax.ShapeDtypeStruct((n, requests, block), bf16), landing),
        in_specs=[smem] * 4 + [hbm] * 6,
        out_specs=(vmem, hbm),
        scratch_shapes=[
            pltpu.VMEM((pages + 1, page_size, width), bf16),
            pltpu.VMEM((n, slots, cap, page_size, width), bf16),
            pltpu.VMEM((requests, rows), bf16),
            pltpu.VMEM((slots, requests, group, head_dim), f32),
            pltpu.VMEM((slots, requests, width), bf16),
            pltpu.VMEM((slots, requests, width), f32),
            pltpu.VMEM((slots, pool_pages, page_size, width), bf16),
            pltpu.VMEM((requests, model), bf16),
            pltpu.VMEM((model // chunk, rows, chunk), bf16),
            pltpu.VMEM((slots, requests, group, head_dim), f32),
            pltpu.VMEM((requests, rows), bf16),
            pltpu.VMEM((n, requests, block), bf16),
            pltpu.VMEM((n, requests, block), bf16),
            dma((4,)),
            dma((slots,)),
            dma((model // chunk,)),
            dma((slots,)),
            dma((n, slots, cap)),
            dma((n, slots, cap)),
            dma((n,)),
            dma((n,)),
            dma((n,)),
            dma((n,)),
        ],
        compiler_params=pltpu.CompilerParams(
            collective_id=0, has_side_effects=True, vmem_limit_bytes=60 * 1024 * 1024
        ),
        name="decode_step",
    )(
        page_counts,
        last_fill,
        page_order,
        routes.reshape(1, pages),
        queries,
        new_kv,
        kv_pool,
        hidden,
        out_weight,
        sectioned,
    )
    return pl.pallas_call(
        finish_kernel,
        out_shape=(
            jax.ShapeDtypeStruct((requests, model), bf16),
            jax.ShapeDtypeStruct((requests, model), bf16),
            landing,
        ),
        in_specs=[hbm, hbm, hbm],
        out_specs=(vmem, vmem, hbm),
        scratch_shapes=[
            pltpu.VMEM(landing.shape, bf16),
            pltpu.VMEM((n, requests, block), bf16),
            pltpu.VMEM((model,), bf16),
            dma((2, slots)),
            dma((2,)),
        ],
        name="finish",
    )(gathered, norm_gain, landed)


PER_HEAD_CAP = 2


def solution(mesh):
    return jax.shard_map(
        functools.partial(per_device, cap=PER_HEAD_CAP),
        mesh=mesh,
        in_specs=(
            P(("groups", "batch"), "heads"),
            P(("groups", "heads"), "batch", None),
            P(("groups", "heads"), "batch", None, None),
            P(("groups", "batch"), None),
            P(("groups", "batch"), None),
            P(("groups", "batch"), None),
            P(("groups", "batch"), None),
            P("heads", None),
            P(),
            P(("groups", "heads"), "batch", None, None, None),
            P(("groups", "heads"), "batch", None, None),
        ),
        out_specs=(
            P(("groups", "batch"), None),
            P(("groups", "batch"), None),
            P(("groups", "heads"), "batch", None, None, None, None),
        ),
        check_vma=False,
    )
```
